256 devices in a mesh: gx: 16 (over x_lo, y, core), gy: 16 (over x_hi, z).
Axes of the slice: x: 4 (x_hi: 2, x_lo: 2; x = x_hi * 2 + x_lo), y: 4, z: 8, core: 2. Of those that a mesh axis runs over, the one named last changes fastest.
Arguments:
- src_table: bfloat16 [524288, 256], P(('gx', 'gy')), may hold values from -1.5 to 1.5
- src_acc: float32 [524288], P(('gx', 'gy')), may hold values from 0.02 to 0.5
- dst_table: bfloat16 [524288, 256], P(('gx', 'gy')), may hold values from -1.5 to 1.5
- dst_acc: float32 [524288], P(('gx', 'gy')), may hold values from 0.02 to 0.5
- relations: float32 [16, 256], replicated, may hold values from -4 to 4
- rel_acc: float32 [16], replicated, may hold values from 20 to 200
- edge_src: int32 [16, 16, 2, 512], P('gx', 'gy'), may hold values from 0 to 2047
- edge_dst: int32 [16, 16, 2, 512], P('gx', 'gy'), may hold values from 0 to 2047
- edge_rel: int32 [16, 16, 2, 512], P('gx', 'gy'), may hold values from 0 to 15
- negatives: int32 [16, 16, 2, 1, 512], P('gx', 'gy'), may hold values from 0 to 2047
- counts: int32 [16, 16, 2], P('gx', 'gy'), may hold values from 128 to 512
Outputs:
- src_out: bfloat16 [524288, 256], P(('gx', 'gy'))
- src_acc_out: float32 [524288], P(('gx', 'gy'))
- dst_out: bfloat16 [524288, 256], P(('gx', 'gy'))
- dst_acc_out: float32 [524288], P(('gx', 'gy'))
- relations_out: float32 [16, 256], replicated
The draws below stay inside these ranges and needn't reach their ends.
Inputs may be any that keep to these rules, and one draw needn't show every extreme that they name: `edge_src`: row of the source partition of the bucket. `edge_dst`: row of the destination partition of the bucket. `negatives`: row of the destination partition of the bucket. Only the first counts slots of a bucket's edge lists are live.
All inputs are finite; a program needn't handle non-finite values.
Results may differ from the reference program's by a relative error of at most 0.0027.
Values may be sent and summed in bfloat16 or wider, within the bound.
A program may use at most 64 MiB of HBM per device.

```python
import math
import jax
import jax.numpy as jnp
from jax import lax

D = 256
NREL = 16
NEG = 512
STEPS = 2
ROWS = 2048
EDGES = 512
NBLK = 1
SRC_ROWS = 524288
N_GX = 16
N_GY = 16


def with_ends(entries, key, least, top_value):
    shape = entries.shape
    place = [jax.random.randint(jax.random.fold_in(key, axis), (), 0, shape[axis]) for axis in range(len(shape))]
    entries = entries.at[tuple(place)].set(least)
    longest = shape.index(max(shape))
    place[longest] = (place[longest] + 1) % shape[longest]
    return entries.at[tuple(place)].set(top_value)


def shard_levels(key, extent, split, smallest, top_value):
    def one(dim, blocks):
        steps = jax.random.uniform(jax.random.fold_in(jax.random.fold_in(key, 6), dim), (blocks,), jnp.float32, smallest / len(split), top_value / len(split))
        return jnp.repeat(jnp.exp(steps), extent[dim] // blocks).reshape((-1,) + (1,) * (len(extent) - dim - 1))

    gain = one(*split[0])
    for cut in split[1:]:
        gain = gain * one(*cut)
    return gain


def noise(stream_key, shape, deviation, most, cuts=(), kind=jnp.bfloat16):
    values = deviation * jax.random.normal(stream_key, shape, jnp.float32)
    if cuts:
        values = values * shard_levels(stream_key, shape, cuts, -0.22, 0.18)
    return jnp.clip(values, -most, most).astype(kind)


def setup_inputs(seed: int = 0) -> dict:
    splits = jax.random.split(jax.random.key(seed), 12)
    return {
        "src_table": noise(splits[0], (SRC_ROWS, D), 0.25, 1.5, ((0, 256),)),
        "src_acc": jnp.clip(jnp.exp(math.log(0.5) - 3.218876 * jax.random.uniform(splits[1], (SRC_ROWS,), jnp.float32) ** shard_levels(splits[1], (SRC_ROWS,), ((0, 256),), -0.2, 0.2)), 0.02, 0.5),
        "dst_table": noise(splits[2], (SRC_ROWS, D), 0.25, 1.5, ((0, 256),)),
        "dst_acc": jnp.clip(jnp.exp(math.log(0.5) - 3.218876 * jax.random.uniform(splits[3], (SRC_ROWS,), jnp.float32) ** shard_levels(splits[3], (SRC_ROWS,), ((0, 256),), -0.2, 0.2)), 0.02, 0.5),
        "relations": noise(splits[4], (NREL, D), 1.0, 4.0, (), jnp.float32),
        "rel_acc": jnp.clip(jnp.exp(jax.random.uniform(splits[5], (NREL,), jnp.float32, math.log(20.0), math.log(200.0))), 20.0, 200.0),
        "edge_src": with_ends(jax.random.randint(splits[6], (N_GX, N_GY, STEPS, EDGES), 0, ROWS), jax.random.fold_in(splits[6], 1), 0, ROWS - 1).astype(jnp.int32),
        "edge_dst": with_ends(jax.random.randint(splits[7], (N_GX, N_GY, STEPS, EDGES), 0, ROWS), jax.random.fold_in(splits[7], 1), 0, ROWS - 1).astype(jnp.int32),
        "edge_rel": with_ends(jax.random.randint(splits[8], (N_GX, N_GY, STEPS, EDGES), 0, NREL), jax.random.fold_in(splits[8], 1), 0, NREL - 1).astype(jnp.int32),
        "negatives": with_ends(jax.random.randint(splits[9], (N_GX, N_GY, STEPS, NBLK, NEG), 0, ROWS), jax.random.fold_in(splits[9], 1), 0, ROWS - 1).astype(jnp.int32),
        "counts": with_ends(jax.random.randint(splits[10], (N_GX, N_GY, STEPS), EDGES // 4, EDGES + 1), jax.random.fold_in(splits[10], 1), EDGES // 4, EDGES).astype(jnp.int32),
    }


learn_rate = 0.1
relation_rate = 0.5

def bucket_grads(source_rows, dest_slab, relations, dest_ids, rel_ids, negative_ids, live_count, block_count):
    edge_total, columns = source_rows.shape
    block_size = edge_total // negative_ids.shape[0]
    negative_weight = negative_ids.shape[1] ** (-0.5)
    rel_total = relations.shape[0]

    def block_step(number, totals):
        edge_grads, dest_grads, rel_grads = totals
        offset = (number * block_size).astype(jnp.int32)
        source = lax.dynamic_slice_in_dim(source_rows, offset, block_size, 0).astype(jnp.float32)
        dest_block = lax.dynamic_slice_in_dim(dest_ids, offset, block_size, 0)
        rel_block = lax.dynamic_slice_in_dim(rel_ids, offset, block_size, 0)
        negative_rows = lax.dynamic_index_in_dim(negative_ids, number, 0, keepdims=False)
        target = jnp.take(dest_slab, dest_block, axis=0).astype(jnp.float32)
        samples = jnp.take(dest_slab, negative_rows, axis=0)
        onehot = (rel_block[:, None] == jnp.arange(rel_total, dtype=jnp.int32)[None, :]).astype(jnp.float32)
        diagonal = jnp.dot(onehot, relations, precision=lax.Precision.HIGHEST, preferred_element_type=jnp.float32)
        live_mask = (offset + jnp.arange(block_size, dtype=jnp.int32) < live_count).astype(jnp.float32)
        rotated = source * diagonal
        rotated_half = rotated.astype(jnp.bfloat16)
        positive = lax.optimization_barrier(jnp.sum(rotated * target, axis=1))
        scores = lax.dot_general(rotated_half, samples, (((1,), (1,)), ((), ())), preferred_element_type=jnp.float32)
        slopes = (live_mask[:, None] * negative_weight * jax.nn.sigmoid(scores)).astype(jnp.bfloat16)
        pulls = -live_mask * jax.nn.sigmoid(-positive)
        pushes = jnp.dot(slopes, samples, preferred_element_type=jnp.float32)
        upstream = pulls[:, None] * target + pushes
        edge_grads = lax.dynamic_update_slice_in_dim(edge_grads, upstream * diagonal, offset, 0)
        sample_grads = lax.dot_general(slopes, rotated_half, (((0,), (0,)), ((), ())), preferred_element_type=jnp.float32)
        dest_grads = dest_grads.at[dest_block].add(pulls[:, None] * rotated).at[negative_rows].add(sample_grads)
        rel_grads = rel_grads + lax.dot_general(onehot, upstream * source, (((0,), (0,)), ((), ())), precision=lax.Precision.HIGHEST, preferred_element_type=jnp.float32)
        return (edge_grads, dest_grads, rel_grads)
    start_totals = (jnp.zeros((edge_total, columns), jnp.float32), jnp.zeros(dest_slab.shape, jnp.float32), jnp.zeros(relations.shape, jnp.float32))
    return lax.fori_loop(0, block_count, block_step, start_totals)

def adagrad(embedding, accumulator, gradient):
    accum_new = accumulator + lax.optimization_barrier(jnp.mean(gradient * gradient, axis=-1))
    moved = embedding.astype(jnp.float32) - learn_rate * gradient / jnp.sqrt(accum_new)[..., None]
    return (moved.astype(jnp.bfloat16), accum_new)

def reference(src_table, src_acc, dst_table, dst_acc, relations, rel_acc, edge_src, edge_dst, edge_rel, negatives, counts):
    source = src_table.reshape(N_GX, N_GY, ROWS, D)
    source_state = src_acc.reshape(N_GX, N_GY, ROWS)
    target = dst_table.reshape(N_GX, N_GY, ROWS, D)
    target_state = dst_acc.reshape(N_GX, N_GY, ROWS)
    devices_all = N_GX * N_GY
    relation_grad = jnp.zeros((NREL, D), jnp.float32)

    def flatten(array):
        return array.reshape((devices_all,) + array.shape[2:])

    def unflatten(array):
        return array.reshape((N_GX, N_GY) + array.shape[1:])

    def device_work(pieces):
        src_slab, src_state, dst_slab, dst_state, src_ids, dst_ids, rel_ids, neg_ids, live_count = pieces
        picked = jnp.take(src_slab, src_ids, axis=0)
        edge_grads, dest_grads, rel_grads = bucket_grads(picked, dst_slab, relations, dst_ids, rel_ids, neg_ids, live_count, NBLK)
        source_grads = jnp.zeros((ROWS, D), jnp.float32).at[src_ids].add(edge_grads)
        new_src, new_src_state = adagrad(src_slab, src_state, source_grads)
        new_dst, new_dst_state = adagrad(dst_slab, dst_state, dest_grads)
        return (new_src, new_src_state, new_dst, new_dst_state, rel_grads)
    for bucket_step in range(STEPS):
        pieces = (flatten(jnp.roll(source, bucket_step, axis=0)), flatten(jnp.roll(source_state, bucket_step, axis=0)), flatten(jnp.roll(target, bucket_step, axis=1)), flatten(jnp.roll(target_state, bucket_step, axis=1)), flatten(edge_src[:, :, bucket_step]), flatten(edge_dst[:, :, bucket_step]), flatten(edge_rel[:, :, bucket_step]), flatten(negatives[:, :, bucket_step]), flatten(counts[:, :, bucket_step]))
        new_src, new_src_state, new_dst, new_dst_state, rel_grads = lax.map(device_work, pieces)
        source = jnp.roll(unflatten(new_src), -bucket_step, axis=0)
        source_state = jnp.roll(unflatten(new_src_state), -bucket_step, axis=0)
        target = jnp.roll(unflatten(new_dst), -bucket_step, axis=1)
        target_state = jnp.roll(unflatten(new_dst_state), -bucket_step, axis=1)
        relation_grad = relation_grad + lax.optimization_barrier(jnp.sum(rel_grads, axis=0))
    relation_state = rel_acc + lax.optimization_barrier(jnp.mean(relation_grad * relation_grad, axis=1))
    relations_out = relations - relation_rate * relation_grad / jnp.sqrt(relation_state)[:, None]
    return (source.reshape(SRC_ROWS, D), source_state.reshape(SRC_ROWS), target.reshape(SRC_ROWS, D), target_state.reshape(SRC_ROWS), relations_out)
```

```python
import functools

import jax
import jax.numpy as jnp
from jax import lax
from jax.experimental import pallas as pl
from jax.experimental.pallas import tpu as pltpu
from jax.sharding import PartitionSpec as P

MESH = pl.DeviceIdType.MESH
bf16, f32, i32 = jnp.bfloat16, jnp.float32, jnp.int32

learn_rate = 0.1
relation_rate = 0.5
CHUNKS = 4
BLOCK = 256
LANES = 128
SRC, DST, REL, NEGS = 0, 1, 2, 3
NT = (((1,), (1,)), ((), ()))
TN = (((0,), (0,)), ((), ()))


def mm(a, b, dims=(((1,), (0,)), ((), ()))):
    return lax.dot_general(a, b, dims, preferred_element_type=f32)


def ones_where(mask):
    return jnp.where(mask, 1.0, 0.0).astype(bf16)


def kernel(
    shape,
    src_hbm, src_acc, dst_hbm, dst_acc, relations, rel_acc, edge_src, edge_dst, edge_rel, negatives, counts,
    src_out, src_acc_out, dst_out, dst_acc_out, rel_out,
    src_tab, dst_tab, src_state, dst_state,
    pack_mine, pack_run, pack_own, cols,
    rel_parts, source, targets, edge_grads, dest_vals, rotated_half, slopes, up_source,
    send_rows, recv_rows, home_grads,
    rel_sum, part, row_buf, col_buf, all_buf, rel_total,
    load_sem, out_sem, idx_send, idx_recv, row_send, row_recv, ret_send, ret_recv, red_send, red_recv,
):
    nx, ny = shape
    rows, width = src_tab.shape
    edges = edge_src.shape[1]
    negs = negatives.shape[1]
    rels = relations.shape[0]
    chunk = edges // CHUNKS
    blocks = rows // BLOCK
    weight = negs ** (-0.5)
    gx, gy = lax.axis_index("gx"), lax.axis_index("gy")

    def peer(dx, dy):
        return (lax.rem(gx + (dx % nx), nx), lax.rem(gy + (dy % ny), ny))

    load_src = pltpu.make_async_copy(src_hbm, src_tab, load_sem.at[0])
    load_dst = pltpu.make_async_copy(dst_hbm, dst_tab, load_sem.at[1])
    load_src.start()
    load_dst.start()

    barrier = pltpu.get_barrier_semaphore()
    partners = [peer(k, 0) for k in range(1, nx)] + [peer(0, k) for k in range(1, ny)]
    partners += [peer(1, -1), peer(-1, 1)]
    for device in partners:
        pl.semaphore_signal(barrier, inc=1, device_id=device, device_id_type=MESH)

    lane = lax.broadcasted_iota(i32, (1, edges), 1)
    for t in range(2):
        pack_mine[4 * t + SRC : 4 * t + SRC + 1, :] = edge_src[t : t + 1, :]
        pack_mine[4 * t + DST : 4 * t + DST + 1, :] = edge_dst[t : t + 1, :]
        pack_mine[4 * t + REL : 4 * t + REL + 1, :] = jnp.where(lane < counts[t], edge_rel[t : t + 1, :], -1)
        pack_mine[4 * t + NEGS : 4 * t + NEGS + 1, :] = negatives[t : t + 1, :]

    rel = relations[...]
    rel_hi = rel.astype(bf16)
    rest = rel - rel_hi.astype(f32)
    rel_mid = rest.astype(bf16)
    rel_low = (rest - rel_mid.astype(f32)).astype(bf16)
    rel_parts[...] = jnp.zeros_like(rel_parts)
    rel_parts[0:rels, :] = rel_hi
    rel_parts[rels : 2 * rels, :] = rel_mid
    rel_parts[2 * rels : 3 * rels, :] = rel_low

    def gather(ids, table):
        spots = lax.broadcasted_iota(i32, (ids.shape[0], rows), 1)
        return mm(ones_where(ids == spots), table[...]).astype(bf16)

    def bucket_chunk(c, from_rows, col):
        at = pl.ds(c * chunk, chunk)
        s = from_rows[at, :].astype(f32)
        d = targets[at, :].astype(f32)
        kind = cols[at, col + REL : col + REL + 1]
        spots = lax.broadcasted_iota(i32, (chunk, rel_parts.shape[0]), 1)
        diagonal = mm(ones_where((spots & (rels - 1)) == kind), rel_parts[...])
        rotated = s * diagonal
        half = rotated.astype(bf16)
        positive = jnp.sum(rotated * d, axis=1, keepdims=True)
        live = jnp.where(kind >= 0, 0.5, 0.0)
        samples = targets[edges:, :]
        scores = mm(half, samples, NT)
        slope = ((live * weight) * (1.0 + jnp.tanh(0.5 * scores))).astype(bf16)
        pulls = -live * (1.0 - jnp.tanh(0.5 * positive))
        upstream = pulls * d + mm(slope, samples)
        edge_grads[at, :] = (upstream * diagonal).astype(bf16)
        dest_vals[at, :] = (pulls * rotated).astype(bf16)
        rotated_half[at, :] = half
        slopes[at, :] = slope
        product = upstream * s
        high = product.astype(bf16)
        up_source[at, 0:width] = high
        up_source[at, width:] = (product - high.astype(f32)).astype(bf16)

    def relation_grad(pack, row):
        kinds = lax.broadcasted_iota(i32, (rels, edges), 0)
        both = mm(ones_where(kinds == pack[row + REL : row + REL + 1, :]), up_source[...])
        return both[:, 0:width] + both[:, width:]

    def negative_grads():
        dest_vals[edges:, :] = mm(slopes[...], rotated_half[...], TN).astype(bf16)

    eye = lax.broadcasted_iota(i32, (LANES, LANES), 0) == lax.broadcasted_iota(i32, (LANES, LANES), 1)

    def update(table, acc_in, acc_new, terms, out=None, sems=None):
        def step(b, carry):
            first = pl.multiple_of(b * BLOCK, BLOCK)
            grad = None
            for ids, values in terms:
                spots = lax.broadcasted_iota(i32, (BLOCK, ids.shape[1]), 0) + first
                term = mm(ones_where(spots == ids), values())
                grad = term if grad is None else grad + term
            for h in range(BLOCK // LANES):
                g = grad[h * LANES : (h + 1) * LANES, :]
                line = pl.ds(b * (BLOCK // LANES) + h, 1)
                squares = g * g
                both = squares[:, 0:LANES] + squares[:, LANES:]
                mixed = both * (1.0 / width) + jnp.where(eye, acc_in[line, :], 0.0)
                state = jnp.sum(mixed, axis=1, keepdims=True)
                acc_new[line, :] = jnp.sum(jnp.where(eye, state, 0.0), axis=0, keepdims=True)
                at = pl.ds(first + h * LANES, LANES)
                moved = table[at, :].astype(f32) - g * (learn_rate * lax.rsqrt(state))
                table[at, :] = moved.astype(bf16)
            if out is not None:
                here = pl.ds(first, BLOCK)
                pltpu.make_async_copy(table.at[here, :], out.at[here, :], sems.at[b]).start()
            return carry

        lax.fori_loop(0, blocks, step, 0)

    def finish(table, out, sems):
        for b in range(blocks):
            here = pl.ds(b * BLOCK, BLOCK)
            pltpu.make_async_copy(table.at[here, :], out.at[here, :], sems.at[b]).wait()

    cols[...] = pack_mine[...].T
    load_src.wait()
    source[...] = gather(cols[:, SRC : SRC + 1], src_tab)
    load_dst.wait()
    targets[0:edges, :] = gather(cols[:, DST : DST + 1], dst_tab)
    targets[edges:, :] = gather(cols[:, NEGS : NEGS + 1], dst_tab)
    for c in range(CHUNKS):
        bucket_chunk(c, source, 0)
    rel_sum[...] = relation_grad(pack_mine, 0)

    pl.semaphore_wait(barrier, len(partners))
    to_run = pltpu.make_async_remote_copy(
        src_ref=pack_mine, dst_ref=pack_run, send_sem=idx_send.at[0], recv_sem=idx_recv.at[0],
        device_id=peer(0, -1), device_id_type=MESH,
    )
    to_own = pltpu.make_async_remote_copy(
        src_ref=pack_mine, dst_ref=pack_own, send_sem=idx_send.at[1], recv_sem=idx_recv.at[1],
        device_id=peer(-1, 0), device_id_type=MESH,
    )
    to_own.start()
    to_run.start()

    update(src_tab, src_acc, src_state, [(pack_mine[SRC : SRC + 1, :], lambda: edge_grads[...])])

    to_own.wait()
    cols[...] = pack_own[...].T

    def row_copy(c):
        at = pl.ds(c * chunk, chunk)
        return pltpu.make_async_remote_copy(
            src_ref=send_rows.at[at, :], dst_ref=recv_rows.at[at, :], send_sem=row_send.at[c], recv_sem=row_recv.at[c],
            device_id=peer(1, -1), device_id_type=MESH,
        )

    def home_copy(c):
        at = pl.ds(c * chunk, chunk)
        return pltpu.make_async_remote_copy(
            src_ref=edge_grads.at[at, :], dst_ref=home_grads.at[at, :], send_sem=ret_send.at[c], recv_sem=ret_recv.at[c],
            device_id=peer(-1, 1), device_id_type=MESH,
        )

    for c in range(0, CHUNKS, 2):
        both = gather(cols[c * chunk : (c + 2) * chunk, 4 + SRC : 5 + SRC], src_tab)
        send_rows[c * chunk : (c + 2) * chunk, :] = both
        row_copy(c).start()
        row_copy(c + 1).start()

    negative_grads()
    dest_terms = lambda pack, row: [
        (pack[row + DST : row + DST + 1, :], lambda: dest_vals[0:edges, :]),
        (pack[row + NEGS : row + NEGS + 1, :], lambda: dest_vals[edges:, :]),
    ]
    update(dst_tab, dst_acc, dst_state, dest_terms(pack_mine, 0))
    to_run.wait()
    cols[...] = pack_run[...].T
    targets[0:edges, :] = gather(cols[:, 4 + DST : 5 + DST], dst_tab)
    targets[edges:, :] = gather(cols[:, 4 + NEGS : 5 + NEGS], dst_tab)

    for c in range(CHUNKS):
        row_copy(c).wait()
        bucket_chunk(c, recv_rows, 4)
        home_copy(c).start()
    total = rel_sum[...] + relation_grad(pack_run, 4)
    for i in range(rels):
        part[i] = total[i : i + 1, :]

    def scatter_copy(k):
        to = lax.rem(gx + k, nx)
        return pltpu.make_async_remote_copy(
            src_ref=part.at[to], dst_ref=row_buf.at[gx], send_sem=red_send.at[0, k], recv_sem=red_recv.at[0, k],
            device_id=(to, gy), device_id_type=MESH,
        )

    def cross_copy(k):
        to = lax.rem(gy + k, ny)
        return pltpu.make_async_remote_copy(
            src_ref=col_buf.at[gy], dst_ref=col_buf.at[gy], send_sem=red_send.at[1, k], recv_sem=red_recv.at[1, k],
            device_id=(gx, to), device_id_type=MESH,
        )

    def spread_copy(k):
        to = lax.rem(gx + k, nx)
        return pltpu.make_async_remote_copy(
            src_ref=all_buf.at[gx], dst_ref=all_buf.at[gx], send_sem=red_send.at[2, k], recv_sem=red_recv.at[2, k],
            device_id=(to, gy), device_id_type=MESH,
        )

    for k in range(1, nx):
        scatter_copy(k).start()
    row_buf[gx] = part[gx]

    negative_grads()
    update(dst_tab, dst_state, dst_acc_out, dest_terms(pack_run, 4), dst_out, out_sem.at[0])

    for k in range(1, nx):
        scatter_copy(k).wait()
    row = row_buf[0]
    for i in range(1, nx):
        row = row + row_buf[i]
    col_buf[gy] = row
    for k in range(1, ny):
        cross_copy(k).start()

    for c in range(CHUNKS):
        home_copy(c).wait()
    update(
        src_tab, src_state, src_acc_out, [(pack_own[4 + SRC : 5 + SRC, :], lambda: home_grads[...])], src_out, out_sem.at[1]
    )

    for k in range(1, ny):
        cross_copy(k).wait()
    row = col_buf[0]
    for i in range(1, ny):
        row = row + col_buf[i]
    all_buf[gx] = row
    for k in range(1, nx):
        spread_copy(k).start()
    finish(dst_tab, dst_out, out_sem.at[0])
    finish(src_tab, src_out, out_sem.at[1])
    for k in range(1, nx):
        spread_copy(k).wait()
    for i in range(rels):
        rel_total[i : i + 1, :] = all_buf[i]
    grad = rel_total[...]
    corner = lax.broadcasted_iota(i32, (rels, rels), 0) == lax.broadcasted_iota(i32, (rels, rels), 1)
    state = jnp.sum(jnp.where(corner, rel_acc[...], 0.0), axis=1, keepdims=True)
    state = state + jnp.sum(grad * grad, axis=1, keepdims=True) * (1.0 / width)
    rel_out[...] = relations[...] - relation_rate * grad * lax.rsqrt(state)


def solution(mesh):
    nx, ny = mesh.shape["gx"], mesh.shape["gy"]

    def local(src_table, src_acc, dst_table, dst_acc, relations, rel_acc, edge_src, edge_dst, edge_rel, negatives, counts):
        rows, width = src_table.shape
        edges = edge_src.shape[-1]
        negs = negatives.shape[-1]
        rels = relations.shape[0]
        lines = rows // LANES
        vmem = pl.BlockSpec(memory_space=pltpu.VMEM)
        smem = pl.BlockSpec(memory_space=pltpu.SMEM)
        hbm = pl.BlockSpec(memory_space=pl.ANY)
        table = jax.ShapeDtypeStruct((rows, width), bf16)
        state = jax.ShapeDtypeStruct((lines, LANES), f32)
        dma = pltpu.SemaphoreType.DMA
        out = pl.pallas_call(
            functools.partial(kernel, (nx, ny)),
            out_shape=(table, state, table, state, jax.ShapeDtypeStruct((rels, width), f32)),
            in_specs=[hbm, vmem, hbm, vmem, vmem, vmem, vmem, vmem, vmem, vmem, smem],
            out_specs=(hbm, vmem, hbm, vmem, vmem),
            scratch_shapes=[
                pltpu.VMEM((rows, width), bf16),
                pltpu.VMEM((rows, width), bf16),
                pltpu.VMEM((lines, LANES), f32),
                pltpu.VMEM((lines, LANES), f32),
                pltpu.VMEM((8, edges), i32),
                pltpu.VMEM((8, edges), i32),
                pltpu.VMEM((8, edges), i32),
                pltpu.VMEM((edges, 8), i32),
                pltpu.VMEM((LANES, width), bf16),
                pltpu.VMEM((edges, width), bf16),
                pltpu.VMEM((edges + negs, width), bf16),
                pltpu.VMEM((edges, width), bf16),
                pltpu.VMEM((edges + negs, width), bf16),
                pltpu.VMEM((edges, width), bf16),
                pltpu.VMEM((edges, negs), bf16),
                pltpu.VMEM((edges, 2 * width), bf16),
                pltpu.VMEM((edges, width), bf16),
                pltpu.VMEM((edges, width), bf16),
                pltpu.VMEM((edges, width), bf16),
                pltpu.VMEM((rels, width), f32),
                pltpu.VMEM((rels, 1, width), f32),
                pltpu.VMEM((nx, 1, width), f32),
                pltpu.VMEM((ny, 1, width), f32),
                pltpu.VMEM((nx, 1, width), f32),
                pltpu.VMEM((rels, width), f32),
                dma((2,)),
                dma((2, rows // BLOCK)),
                dma((2,)),
                dma((2,)),
                dma((CHUNKS,)),
                dma((CHUNKS,)),
                dma((CHUNKS,)),
                dma((CHUNKS,)),
                dma((3, max(nx, ny))),
                dma((3, max(nx, ny))),
            ],
            compiler_params=pltpu.CompilerParams(collective_id=0, has_side_effects=True, vmem_limit_bytes=48 << 20),
        )(
            src_table,
            src_acc.reshape(lines, LANES),
            dst_table,
            dst_acc.reshape(lines, LANES),
            relations,
            rel_acc.reshape(1, rels),
            edge_src.reshape(2, edges),
            edge_dst.reshape(2, edges),
            edge_rel.reshape(2, edges),
            negatives.reshape(2, negs),
            counts.reshape(2),
        )
        return (out[0], out[1].reshape(rows), out[2], out[3].reshape(rows), out[4])

    both = ("gx", "gy")
    listed = P("gx", "gy", None, None)
    return jax.shard_map(
        local,
        mesh=mesh,
        in_specs=(
            P(both, None), P(both), P(both, None), P(both), P(), P(),
            listed, listed, listed, P("gx", "gy", None, None, None), P("gx", "gy", None),
        ),
        out_specs=(P(both, None), P(both), P(both, None), P(both), P()),
        check_vma=False,
    )
```

```python
import functools

import jax
import jax.numpy as jnp
from jax import lax
from jax.experimental import pallas as pl
from jax.experimental.pallas import tpu as pltpu
from jax.sharding import PartitionSpec as P

MESH = pl.DeviceIdType.MESH
bf16, f32, i32 = jnp.bfloat16, jnp.float32, jnp.int32

learn_rate = 0.1
relation_rate = 0.5
CHUNKS = 4
BLOCK = 256
LANES = 128
SRC, DST, REL, NEGS = 0, 1, 2, 3
NT = (((1,), (1,)), ((), ()))
TN = (((0,), (0,)), ((), ()))


def mm(a, b, dims=(((1,), (0,)), ((), ()))):
    return lax.dot_general(a, b, dims, preferred_element_type=f32)


def ones_where(mask):
    return jnp.where(mask, 1.0, 0.0).astype(bf16)


def kernel(
    shape,
    src_hbm, src_acc_hbm, dst_hbm, dst_acc_hbm, relations_hbm, rel_acc_hbm, edge_src_hbm, edge_dst_hbm, edge_rel_hbm, negatives_hbm,
    counts_hbm,
    src_tab, src_acc_out, dst_tab, dst_acc_out, rel_out,
    src_acc, dst_acc, relations, rel_acc, edge_src, edge_dst, edge_rel, negatives, counts,
    src_state, dst_state,
    pack_mine, pack_run, pack_own, cols,
    rel_parts, acc_parts, source, targets, edge_grads, dest_vals, rotated_half, slopes, up_source,
    send_rows, recv_rows, run_grads, home_grads,
    rel_sum, part, row_buf, col_buf, all_buf, rel_total,
    load_sem, idx_send, idx_recv, row_send, row_recv, ret_send, ret_recv, red_send, red_recv,
):
    nx, ny = shape
    rows, width = src_tab.shape
    lines = rows // LANES
    edges = edge_src.shape[1]
    rels = relations.shape[0]
    chunk = edges // CHUNKS
    blocks = rows // BLOCK
    weight = negatives.shape[-1] ** (-0.5)
    gx, gy = lax.axis_index("gx"), lax.axis_index("gy")
    half_x, half_y = nx // 2, ny // 2

    def peer(dx, dy):
        return (lax.rem(gx + (dx % nx), nx), lax.rem(gy + (dy % ny), ny))

    def near(k):
        return ((gx // half_x) * half_x + lax.rem(gx + k, half_x), gy)

    def far(offset):
        a, b, c = offset
        x = lax.rem(gx // half_x + a, 2) * half_x + lax.rem(gx, half_x)
        y = lax.rem(gy // half_y + b, 2) * half_y + lax.rem(gy + c, half_y)
        return (x, y)

    offsets = [(a, b, c) for a in range(2) for b in range(2) for c in range(half_y)][1:]
    offsets.sort(key=lambda o: -min(o[2], half_y - o[2]) - (2 if o[:2] == (0, 1) else max(o[:2])))

    def loaded(k, source_ref, target_ref):
        return pltpu.make_async_copy(source_ref, target_ref, load_sem.at[k])

    loads = [
        loaded(k, *pair)
        for k, pair in enumerate(
            (
                (edge_src_hbm, edge_src), (edge_dst_hbm, edge_dst), (edge_rel_hbm, edge_rel), (negatives_hbm, negatives),
                (counts_hbm, counts), (relations_hbm, relations), (src_hbm, src_tab), (dst_hbm, dst_tab),
                (src_acc_hbm, src_acc), (dst_acc_hbm, dst_acc), (rel_acc_hbm, rel_acc),
            )
        )
    ]
    for copy in loads:
        copy.start()

    barrier = pltpu.get_barrier_semaphore()
    partners = [far(o) for o in offsets] + [near(k) for k in range(1, half_x)]
    partners += [peer(1, 0), peer(-1, 0), peer(1, -1), peer(-1, 1)]
    if ny > 2:
        partners += [peer(0, 1), peer(0, -1)]
    for device in partners:
        pl.semaphore_signal(barrier, inc=1, device_id=device, device_id_type=MESH)

    for copy in loads[:6]:
        copy.wait()
    lane = lax.broadcasted_iota(i32, (1, edges), 1)
    for t in range(2):
        pack_mine[4 * t + SRC : 4 * t + SRC + 1, :] = edge_src[t : t + 1, :]
        pack_mine[4 * t + DST : 4 * t + DST + 1, :] = edge_dst[t : t + 1, :]
        pack_mine[4 * t + REL : 4 * t + REL + 1, :] = jnp.where(lane < counts[0:1, t : t + 1], edge_rel[t : t + 1, :], -1)
        pack_mine[4 * t + NEGS : 4 * t + NEGS + 1, :] = negatives[t]

    def split(value, parts):
        count = value.shape[0]
        parts[...] = jnp.zeros_like(parts)
        high = value.astype(bf16)
        rest = value - high.astype(f32)
        middle = rest.astype(bf16)
        parts[0:count, :] = high
        parts[count : 2 * count, :] = middle
        parts[2 * count : 3 * count, :] = (rest - middle.astype(f32)).astype(bf16)

    def pick(ids, parts, count):
        spots = lax.broadcasted_iota(i32, (ids.shape[0], parts.shape[0]), 1)
        return mm(ones_where((spots & (count - 1)) == ids), parts[...])

    split(relations[...], rel_parts)

    def gather(ids, table):
        spots = lax.broadcasted_iota(i32, (ids.shape[0], rows), 1)
        return mm(ones_where(ids == spots), table[...]).astype(bf16)

    def bucket_chunk(c, from_rows, col, grads):
        at = pl.ds(c * chunk, chunk)
        s = from_rows[at, :].astype(f32)
        d = targets[at, :].astype(f32)
        kind = cols[at, col + REL : col + REL + 1]
        diagonal = pick(kind, rel_parts, rels)
        rotated = s * diagonal
        half = rotated.astype(bf16)
        positive = jnp.sum(rotated * d, axis=1, keepdims=True)
        live = jnp.where(kind >= 0, 0.5, 0.0)
        samples = targets[edges:, :]
        scores = mm(half, samples, NT)
        slope = ((live * weight) * (1.0 + jnp.tanh(0.5 * scores))).astype(bf16)
        pulls = -live * (1.0 - jnp.tanh(0.5 * positive))
        upstream = pulls * d + mm(slope, samples)
        grads[at, :] = (upstream * diagonal).astype(bf16)
        dest_vals[at, :] = (pulls * rotated).astype(bf16)
        rotated_half[at, :] = half
        slopes[at, :] = slope
        product = upstream * s
        high = product.astype(bf16)
        up_source[at, 0:width] = high
        up_source[at, width:] = (product - high.astype(f32)).astype(bf16)

    def relation_grad(pack, row):
        kinds = lax.broadcasted_iota(i32, (rels, edges), 0)
        both = mm(ones_where(kinds == pack[row + REL : row + REL + 1, :]), up_source[...])
        return both[:, 0:width] + both[:, width:]

    def negative_grads():
        dest_vals[edges:, :] = mm(slopes[...], rotated_half[...], TN).astype(bf16)

    eye = lax.broadcasted_iota(i32, (LANES, LANES), 0) == lax.broadcasted_iota(i32, (LANES, LANES), 1)

    def update(table, acc_in, acc_new, terms):
        def step(b, carry):
            first = pl.multiple_of(b * BLOCK, BLOCK)
            grad = None
            for ids, values in terms:
                spots = lax.broadcasted_iota(i32, (BLOCK, ids.shape[1]), 0) + first
                term = mm(ones_where(spots == ids), values())
                grad = term if grad is None else grad + term
            for h in range(BLOCK // LANES):
                g = grad[h * LANES : (h + 1) * LANES, :]
                line = pl.ds(b * (BLOCK // LANES) + h, 1)
                squares = g * g
                both = squares[:, 0:LANES] + squares[:, LANES:]
                mixed = both * (1.0 / width) + jnp.where(eye, acc_in[line, :], 0.0)
                state = jnp.sum(mixed, axis=1, keepdims=True)
                acc_new[line, :] = jnp.sum(jnp.where(eye, state, 0.0), axis=0, keepdims=True)
                at = pl.ds(first + h * LANES, LANES)
                moved = table[at, :].astype(f32) - g * (learn_rate * lax.rsqrt(state))
                table[at, :] = moved.astype(bf16)
            return carry

        lax.fori_loop(0, blocks, step, 0, unroll=2)

    cols[...] = pack_mine[...].T
    loads[6].wait()
    source[...] = gather(cols[:, SRC : SRC + 1], src_tab)
    loads[7].wait()
    targets[0:edges, :] = gather(cols[:, DST : DST + 1], dst_tab)
    targets[edges:, :] = gather(cols[:, NEGS : NEGS + 1], dst_tab)
    for copy in loads[8:]:
        copy.wait()
    split(src_acc[...], acc_parts)

    pl.semaphore_wait(barrier, len(partners))
    to_own = pltpu.make_async_remote_copy(
        src_ref=pack_mine, dst_ref=pack_own, send_sem=idx_send.at[1], recv_sem=idx_recv.at[1],
        device_id=peer(-1, 0), device_id_type=MESH,
    )
    to_run = pltpu.make_async_remote_copy(
        src_ref=pack_mine, dst_ref=pack_run, send_sem=idx_send.at[0], recv_sem=idx_recv.at[0],
        device_id=peer(0, -1), device_id_type=MESH,
    )
    to_own.start()
    to_run.start()

    for c in range(CHUNKS):
        bucket_chunk(c, source, 0, edge_grads)

    def row_copy(c):
        at = pl.ds(c * chunk, chunk)
        return pltpu.make_async_remote_copy(
            src_ref=send_rows.at[at, :], dst_ref=recv_rows.at[at, :], send_sem=row_send.at[c], recv_sem=row_recv.at[c],
            device_id=peer(1, -1), device_id_type=MESH,
        )

    def home_copy(c):
        at = pl.ds(c * chunk, chunk)
        return pltpu.make_async_remote_copy(
            src_ref=run_grads.at[at, :], dst_ref=home_grads.at[at, :], send_sem=ret_send.at[c], recv_sem=ret_recv.at[c],
            device_id=peer(-1, 1), device_id_type=MESH,
        )

    to_own.wait()
    cols[...] = pack_own[...].T
    source[...] = gather(cols[:, 4 + SRC : 5 + SRC], src_tab)
    for c in range(CHUNKS):
        at = pl.ds(c * chunk, chunk)
        named = cols[at, 4 + SRC : 5 + SRC]
        g = mm(ones_where(named == pack_mine[SRC : SRC + 1, :]), edge_grads[...])
        squares = g * g
        spots = lax.broadcasted_iota(i32, (chunk, LANES), 1)
        accs = pick(named // LANES, acc_parts, lines)
        mixed = (squares[:, 0:LANES] + squares[:, LANES:]) * (1.0 / width) + jnp.where(spots == lax.rem(named, LANES), accs, 0.0)
        state = jnp.sum(mixed, axis=1, keepdims=True)
        send_rows[at, :] = (source[at, :].astype(f32) - g * (learn_rate * lax.rsqrt(state))).astype(bf16)
        row_copy(c).start()

    rel_sum[...] = relation_grad(pack_mine, 0)
    update(src_tab, src_acc, src_state, [(pack_mine[SRC : SRC + 1, :], lambda: edge_grads[...])])
    negative_grads()
    dest_terms = lambda pack, row: [
        (pack[row + DST : row + DST + 1, :], lambda: dest_vals[0:edges, :]),
        (pack[row + NEGS : row + NEGS + 1, :], lambda: dest_vals[edges:, :]),
    ]
    update(dst_tab, dst_acc, dst_state, dest_terms(pack_mine, 0))
    to_run.wait()
    cols[...] = pack_run[...].T
    targets[0:edges, :] = gather(cols[:, 4 + DST : 5 + DST], dst_tab)
    targets[edges:, :] = gather(cols[:, 4 + NEGS : 5 + NEGS], dst_tab)

    for c in range(CHUNKS):
        row_copy(c).wait()
        bucket_chunk(c, recv_rows, 4, run_grads)
        home_copy(c).start()
    total = rel_sum[...] + relation_grad(pack_run, 4)
    each = rels // half_x
    for i in range(half_x):
        part[i] = total[i * each : (i + 1) * each, :]

    place = lax.rem(gx, half_x)
    mine = (gx // half_x) * ny + gy

    def scatter_copy(k):
        device = near(k)
        return pltpu.make_async_remote_copy(
            src_ref=part.at[lax.rem(device[0], half_x)], dst_ref=row_buf.at[place],
            send_sem=red_send.at[0, k], recv_sem=red_recv.at[0, k], device_id=device, device_id_type=MESH,
        )

    def cross_copy(k):
        return pltpu.make_async_remote_copy(
            src_ref=col_buf.at[mine], dst_ref=col_buf.at[mine],
            send_sem=red_send.at[1, k], recv_sem=red_recv.at[1, k], device_id=far(offsets[k]), device_id_type=MESH,
        )

    def spread_copy(k):
        return pltpu.make_async_remote_copy(
            src_ref=all_buf.at[place], dst_ref=all_buf.at[place],
            send_sem=red_send.at[2, k], recv_sem=red_recv.at[2, k], device_id=near(k), device_id_type=MESH,
        )

    nears, fars = range(1, half_x), range(len(offsets))
    for k in nears:
        scatter_copy(k).start()
    row_buf[place] = part[place]
    negative_grads()
    for k in nears:
        scatter_copy(k).wait()
    row = row_buf[0]
    for i in range(1, half_x):
        row = row + row_buf[i]
    col_buf[mine] = row
    for k in fars:
        cross_copy(k).start()

    update(dst_tab, dst_state, dst_acc_out, dest_terms(pack_run, 4))

    for c in range(CHUNKS):
        home_copy(c).wait()
    update(src_tab, src_state, src_acc_out, [(pack_own[4 + SRC : 5 + SRC, :], lambda: home_grads[...])])

    for k in fars:
        cross_copy(k).wait()
    row = col_buf[0]
    for i in range(1, 2 * ny):
        row = row + col_buf[i]
    all_buf[place] = row
    for k in nears:
        spread_copy(k).start()
    for k in nears:
        spread_copy(k).wait()
    for i in range(half_x):
        rel_total[i * each : (i + 1) * each, :] = all_buf[i]
    grad = rel_total[...]
    corner = lax.broadcasted_iota(i32, (rels, rels), 0) == lax.broadcasted_iota(i32, (rels, rels), 1)
    state = jnp.sum(jnp.where(corner, rel_acc[...], 0.0), axis=1, keepdims=True)
    state = state + jnp.sum(grad * grad, axis=1, keepdims=True) * (1.0 / width)
    rel_out[...] = relations[...] - relation_rate * grad * lax.rsqrt(state)


def store(*refs):
    count = len(refs) // 2
    sems = refs[-1]
    copies = [pltpu.make_async_copy(refs[i], refs[count + i], sems.at[i]) for i in range(count)]
    for copy in copies:
        copy.start()
    for copy in copies:
        copy.wait()


def solution(mesh):
    nx, ny = mesh.shape["gx"], mesh.shape["gy"]

    def local(src_table, src_acc, dst_table, dst_acc, relations, rel_acc, edge_src, edge_dst, edge_rel, negatives, counts):
        rows, width = src_table.shape
        edges = edge_src.shape[-1]
        negs = negatives.shape[-1]
        rels = relations.shape[0]
        lines = rows // LANES
        vmem = pl.BlockSpec(memory_space=pltpu.VMEM)
        hbm = pl.BlockSpec(memory_space=pltpu.HBM)
        table = jax.ShapeDtypeStruct((rows, width), bf16)
        state = jax.ShapeDtypeStruct((lines, LANES), f32)
        outs = (table, state, table, state, jax.ShapeDtypeStruct((rels, width), f32))
        dma = pltpu.SemaphoreType.DMA
        half, far, each = nx // 2, 2 * ny, rels // (nx // 2)
        inner = pl.pallas_call(
            functools.partial(kernel, (nx, ny)),
            out_shape=outs,
            in_specs=[hbm] * 11,
            out_specs=(vmem,) * 5,
            scratch_shapes=[
                pltpu.VMEM((lines, LANES), f32),
                pltpu.VMEM((lines, LANES), f32),
                pltpu.VMEM((rels, width), f32),
                pltpu.VMEM((1, rels), f32),
                pltpu.VMEM((2, edges), i32),
                pltpu.VMEM((2, edges), i32),
                pltpu.VMEM((2, edges), i32),
                pltpu.VMEM((2, 1, negs), i32),
                pltpu.VMEM((1, 2), i32),
                pltpu.VMEM((lines, LANES), f32),
                pltpu.VMEM((lines, LANES), f32),
                pltpu.VMEM((8, edges), i32),
                pltpu.VMEM((8, edges), i32),
                pltpu.VMEM((8, edges), i32),
                pltpu.VMEM((edges, 8), i32),
                pltpu.VMEM((LANES, width), bf16),
                pltpu.VMEM((LANES, LANES), bf16),
                pltpu.VMEM((edges, width), bf16),
                pltpu.VMEM((edges + negs, width), bf16),
                pltpu.VMEM((edges, width), bf16),
                pltpu.VMEM((edges + negs, width), bf16),
                pltpu.VMEM((edges, width), bf16),
                pltpu.VMEM((edges, negs), bf16),
                pltpu.VMEM((edges, 2 * width), bf16),
                pltpu.VMEM((edges, width), bf16),
                pltpu.VMEM((edges, width), bf16),
                pltpu.VMEM((edges, width), bf16),
                pltpu.VMEM((edges, width), bf16),
                pltpu.VMEM((rels, width), f32),
                pltpu.VMEM((half, each, width), f32),
                pltpu.VMEM((half, each, width), f32),
                pltpu.VMEM((far, each, width), f32),
                pltpu.VMEM((half, each, width), f32),
                pltpu.VMEM((rels, width), f32),
                dma((11,)),
                dma((2,)),
                dma((2,)),
                dma((CHUNKS,)),
                dma((CHUNKS,)),
                dma((CHUNKS,)),
                dma((CHUNKS,)),
                dma((3, far)),
                dma((3, far)),
            ],
            compiler_params=pltpu.CompilerParams(collective_id=0, has_side_effects=True, vmem_limit_bytes=40 << 20),
        )(
            *(
                pltpu.with_memory_space_constraint(value, pltpu.HBM)
                for value in (
                    src_table,
                    src_acc.reshape(lines, LANES),
                    dst_table,
                    dst_acc.reshape(lines, LANES),
                    relations,
                    rel_acc.reshape(1, rels),
                    edge_src.reshape(2, edges),
                    edge_dst.reshape(2, edges),
                    edge_rel.reshape(2, edges),
                    negatives.reshape(2, 1, negs),
                    counts.reshape(1, 2),
                )
            )
        )
        out = pl.pallas_call(
            store,
            out_shape=outs,
            in_specs=[vmem] * 5,
            out_specs=(hbm,) * 5,
            scratch_shapes=[dma((5,))],
            compiler_params=pltpu.CompilerParams(vmem_limit_bytes=1 << 20),
        )(*inner)
        return (out[0], out[1].reshape(rows), out[2], out[3].reshape(rows), out[4])

    both = ("gx", "gy")
    listed = P("gx", "gy", None, None)
    return jax.shard_map(
        local,
        mesh=mesh,
        in_specs=(
            P(both, None), P(both), P(both, None), P(both), P(), P(),
            listed, listed, listed, P("gx", "gy", None, None, None), P("gx", "gy", None),
        ),
        out_specs=(P(both, None), P(both), P(both, None), P(both), P()),
        check_vma=False,
    )
```

```python
import functools

import jax
import jax.numpy as jnp
from jax import lax
from jax.experimental import pallas as pl
from jax.experimental.pallas import tpu as pltpu
from jax.sharding import PartitionSpec as P

MESH = pl.DeviceIdType.MESH
bf16, f32, i32 = jnp.bfloat16, jnp.float32, jnp.int32

learn_rate = 0.1
relation_rate = 0.5
CHUNKS = 4
BLOCK = 256
UNROLL = 2
FIRST = 256
LANES = 128
SRC, DST, REL, NEGS = 0, 1, 2, 3
NT = (((1,), (1,)), ((), ()))
TN = (((0,), (0,)), ((), ()))


def mm(a, b, dims=(((1,), (0,)), ((), ()))):
    return lax.dot_general(a, b, dims, preferred_element_type=f32)


def ones_where(mask):
    return jnp.where(mask, 1.0, 0.0).astype(bf16)


def kernel(
    shape,
    src_hbm, src_acc_hbm, dst_hbm, dst_acc_hbm, relations_hbm, rel_acc_hbm, edge_src_hbm, edge_dst_hbm, edge_rel_hbm, negatives_hbm,
    counts_hbm,
    src_tab, src_acc_out, dst_tab, dst_acc_out, rel_out,
    src_acc, dst_acc, relations, rel_acc, edge_src, edge_dst, edge_rel, negatives, counts,
    src_state, dst_state,
    pack_mine, pack_run, pack_own, cols,
    rel_parts, acc_parts, source, targets, edge_grads, dest_vals, rotated_half, slopes, up_source,
    send_rows, recv_rows, run_grads, home_grads,
    rel_sum, part, row_buf, col_buf, all_buf, rel_total,
    load_sem, met, idx_send, idx_recv, row_send, row_recv, ret_send, ret_recv, red_send, red_recv,
):
    nx, ny = shape
    rows, width = src_tab.shape
    lines = rows // LANES
    edges = edge_src.shape[1]
    rels = relations.shape[0]
    chunk = edges // CHUNKS
    blocks = rows // BLOCK
    weight = negatives.shape[-1] ** (-0.5)
    gx, gy = lax.axis_index("gx"), lax.axis_index("gy")
    half_x, half_y = nx // 2, ny // 2

    def peer(dx, dy):
        return (lax.rem(gx + (dx % nx), nx), lax.rem(gy + (dy % ny), ny))

    def near(k):
        return ((gx // half_x) * half_x + lax.rem(gx + k, half_x), gy)

    def far(offset):
        a, b, c = offset
        x = lax.rem(gx // half_x + a, 2) * half_x + lax.rem(gx, half_x)
        y = lax.rem(gy // half_y + b, 2) * half_y + lax.rem(gy + c, half_y)
        return (x, y)

    offsets = [(a, b, c) for a in range(2) for b in range(2) for c in range(half_y)][1:]
    offsets.sort(key=lambda o: -min(o[2], half_y - o[2]) - (2 if o[:2] == (0, 1) else max(o[:2])))

    def loaded(k, source_ref, target_ref):
        return pltpu.make_async_copy(source_ref, target_ref, load_sem.at[k])

    loads = [
        loaded(k, *pair)
        for k, pair in enumerate(
            (
                (edge_src_hbm, edge_src), (edge_dst_hbm, edge_dst), (edge_rel_hbm, edge_rel), (negatives_hbm, negatives),
                (counts_hbm, counts), (relations_hbm, relations), (src_hbm, src_tab), (dst_hbm, dst_tab),
                (src_acc_hbm, src_acc), (dst_acc_hbm, dst_acc), (rel_acc_hbm, rel_acc),
            )
        )
    ]
    for copy in loads:
        copy.start()

    barrier = pltpu.get_barrier_semaphore()
    partners = [peer(1, 0), peer(-1, 0), peer(0, 1), peer(0, -1), peer(1, -1), peer(-1, 1)]
    for device in partners:
        pl.semaphore_signal(barrier, inc=1, device_id=device, device_id_type=MESH)

    def greet(k, devices):
        for device in devices:
            pl.semaphore_signal(met.at[k], inc=1, device_id=device, device_id_type=MESH)

    def greet_both(k, step):
        greet(k, [peer(step, 0), peer(-step, 0)])
        greet(k + 3, [peer(0, step), peer(0, -step)])

    def met_both(k):
        pl.semaphore_wait(met.at[k], 2)
        pl.semaphore_wait(met.at[k + 3], 2)

    for copy in loads[:6]:
        copy.wait()
    lane = lax.broadcasted_iota(i32, (1, edges), 1)
    for t in range(2):
        pack_mine[4 * t + SRC : 4 * t + SRC + 1, :] = edge_src[t : t + 1, :]
        pack_mine[4 * t + DST : 4 * t + DST + 1, :] = edge_dst[t : t + 1, :]
        pack_mine[4 * t + REL : 4 * t + REL + 1, :] = jnp.where(lane < counts[0:1, t : t + 1], edge_rel[t : t + 1, :], -1)
        pack_mine[4 * t + NEGS : 4 * t + NEGS + 1, :] = negatives[t]

    def split(value, parts):
        count = value.shape[0]
        parts[...] = jnp.zeros_like(parts)
        high = value.astype(bf16)
        rest = value - high.astype(f32)
        middle = rest.astype(bf16)
        parts[0:count, :] = high
        parts[count : 2 * count, :] = middle
        parts[2 * count : 3 * count, :] = (rest - middle.astype(f32)).astype(bf16)

    def pick(ids, parts, count):
        spots = lax.broadcasted_iota(i32, (ids.shape[0], parts.shape[0]), 1)
        return mm(ones_where((spots & (count - 1)) == ids), parts[...])

    split(relations[...], rel_parts)

    def gather(ids, table):
        spots = lax.broadcasted_iota(i32, (ids.shape[0], rows), 1)
        return mm(ones_where(ids == spots), table[...]).astype(bf16)

    def bucket_chunk(first, count, from_rows, col, grads):
        at = pl.ds(first, count)
        s = from_rows[at, :].astype(f32)
        d = targets[at, :].astype(f32)
        kind = cols[at, col + REL : col + REL + 1]
        diagonal = pick(kind, rel_parts, rels)
        rotated = s * diagonal
        half = rotated.astype(bf16)
        positive = jnp.sum(rotated * d, axis=1, keepdims=True)
        live = jnp.where(kind >= 0, 0.5, 0.0)
        samples = targets[edges:, :]
        scores = mm(half, samples, NT)
        slope = ((live * weight) * (1.0 + jnp.tanh(0.5 * scores))).astype(bf16)
        pulls = -live * (1.0 - jnp.tanh(0.5 * positive))
        upstream = pulls * d + mm(slope, samples)
        grads[at, :] = (upstream * diagonal).astype(bf16)
        dest_vals[at, :] = (pulls * rotated).astype(bf16)
        rotated_half[at, :] = half
        slopes[at, :] = slope
        product = upstream * s
        high = product.astype(bf16)
        up_source[at, 0:width] = high
        up_source[at, width:] = (product - high.astype(f32)).astype(bf16)

    def relation_grad(pack, row):
        kinds = lax.broadcasted_iota(i32, (rels, edges), 0)
        both = mm(ones_where(kinds == pack[row + REL : row + REL + 1, :]), up_source[...])
        return both[:, 0:width] + both[:, width:]

    def negative_grads():
        dest_vals[edges:, :] = mm(slopes[...], rotated_half[...], TN).astype(bf16)

    eye = lax.broadcasted_iota(i32, (LANES, LANES), 0) == lax.broadcasted_iota(i32, (LANES, LANES), 1)

    def update(table, acc_in, acc_new, terms, begin=0, end=None):
        def step(b, carry):
            first = pl.multiple_of(b * BLOCK, BLOCK)
            grad = None
            for ids, values in terms:
                spots = lax.broadcasted_iota(i32, (BLOCK, ids.shape[1]), 0) + first
                term = mm(ones_where(spots == ids), values())
                grad = term if grad is None else grad + term
            for h in range(BLOCK // LANES):
                g = grad[h * LANES : (h + 1) * LANES, :]
                line = pl.ds(b * (BLOCK // LANES) + h, 1)
                squares = g * g
                both = squares[:, 0:LANES] + squares[:, LANES:]
                mixed = both * (1.0 / width) + jnp.where(eye, acc_in[line, :], 0.0)
                state = jnp.sum(mixed, axis=1, keepdims=True)
                acc_new[line, :] = jnp.sum(jnp.where(eye, state, 0.0), axis=0, keepdims=True)
                at = pl.ds(first + h * LANES, LANES)
                moved = table[at, :].astype(f32) - g * (learn_rate * lax.rsqrt(state))
                table[at, :] = moved.astype(bf16)
            return carry

        lax.fori_loop(begin, blocks if end is None else end, step, 0, unroll=UNROLL)

    cols[...] = pack_mine[...].T
    loads[6].wait()
    source[...] = gather(cols[:, SRC : SRC + 1], src_tab)

    pl.semaphore_wait(barrier, len(partners))
    to_own = pltpu.make_async_remote_copy(
        src_ref=pack_mine, dst_ref=pack_own, send_sem=idx_send.at[1], recv_sem=idx_recv.at[1],
        device_id=peer(-1, 0), device_id_type=MESH,
    )
    to_run = pltpu.make_async_remote_copy(
        src_ref=pack_mine, dst_ref=pack_run, send_sem=idx_send.at[0], recv_sem=idx_recv.at[0],
        device_id=peer(0, -1), device_id_type=MESH,
    )
    to_own.start()
    to_run.start()
    greet_both(0, 1)

    loads[7].wait()
    targets[0:edges, :] = gather(cols[:, DST : DST + 1], dst_tab)
    targets[edges:, :] = gather(cols[:, NEGS : NEGS + 1], dst_tab)
    for copy in loads[8:]:
        copy.wait()
    split(src_acc[...], acc_parts)
    for first in range(0, edges, FIRST):
        bucket_chunk(first, FIRST, source, 0, edge_grads)
    met_both(0)
    greet_both(1, 2)

    def row_copy(c):
        at = pl.ds(c * chunk, chunk)
        return pltpu.make_async_remote_copy(
            src_ref=send_rows.at[at, :], dst_ref=recv_rows.at[at, :], send_sem=row_send.at[c], recv_sem=row_recv.at[c],
            device_id=peer(1, -1), device_id_type=MESH,
        )

    def home_copy(c):
        at = pl.ds(c * chunk, chunk)
        return pltpu.make_async_remote_copy(
            src_ref=run_grads.at[at, :], dst_ref=home_grads.at[at, :], send_sem=ret_send.at[c], recv_sem=ret_recv.at[c],
            device_id=peer(-1, 1), device_id_type=MESH,
        )

    to_own.wait()
    cols[...] = pack_own[...].T
    source[...] = gather(cols[:, 4 + SRC : 5 + SRC], src_tab)
    for c in range(CHUNKS):
        at = pl.ds(c * chunk, chunk)
        named = cols[at, 4 + SRC : 5 + SRC]
        g = mm(ones_where(named == pack_mine[SRC : SRC + 1, :]), edge_grads[...])
        squares = g * g
        spots = lax.broadcasted_iota(i32, (chunk, LANES), 1)
        accs = pick(named // LANES, acc_parts, lines)
        mixed = (squares[:, 0:LANES] + squares[:, LANES:]) * (1.0 / width) + jnp.where(spots == lax.rem(named, LANES), accs, 0.0)
        state = jnp.sum(mixed, axis=1, keepdims=True)
        send_rows[at, :] = (source[at, :].astype(f32) - g * (learn_rate * lax.rsqrt(state))).astype(bf16)
        row_copy(c).start()

    rel_sum[...] = relation_grad(pack_mine, 0)
    negative_grads()
    met_both(1)
    greet_both(2, 4)
    dest_terms = lambda pack, row: [
        (pack[row + DST : row + DST + 1, :], lambda: dest_vals[0:edges, :]),
        (pack[row + NEGS : row + NEGS + 1, :], lambda: dest_vals[edges:, :]),
    ]
    update(dst_tab, dst_acc, dst_state, dest_terms(pack_mine, 0))
    met_both(2)
    greet(6, [peer(half_x, 0)])
    to_run.wait()
    cols[...] = pack_run[...].T
    targets[0:edges, :] = gather(cols[:, 4 + DST : 5 + DST], dst_tab)
    targets[edges:, :] = gather(cols[:, 4 + NEGS : 5 + NEGS], dst_tab)

    cuts = (0, 2, 4, blocks, blocks)
    for c in range(CHUNKS):
        row_copy(c).wait()
        bucket_chunk(c * chunk, chunk, recv_rows, 4, run_grads)
        home_copy(c).start()
        if cuts[c] < cuts[c + 1]:
            terms = [(pack_mine[SRC : SRC + 1, :], lambda: edge_grads[...])]
            update(src_tab, src_acc, src_state, terms, cuts[c], cuts[c + 1])
    pl.semaphore_wait(met.at[6], 1)
    total = rel_sum[...] + relation_grad(pack_run, 4)
    each = rels // half_x
    for i in range(half_x):
        part[i] = total[i * each : (i + 1) * each, :]

    place = lax.rem(gx, half_x)
    mine = (gx // half_x) * ny + gy

    def exchange(phase, source_ref, target_ref, device):
        pltpu.make_async_remote_copy(
            src_ref=source_ref, dst_ref=target_ref, send_sem=red_send.at[phase], recv_sem=red_recv.at[phase],
            device_id=device, device_id_type=MESH,
        ).start()

    def all_of(sem, phase, buf, count):
        ref = buf.at[pl.ds(0, count)]
        pltpu.make_async_copy(ref, ref, sem.at[phase]).wait()

    def added(buf):
        terms = [buf[i] for i in range(buf.shape[0])]
        while len(terms) > 1:
            terms = [terms[i] + terms[i + 1] for i in range(0, len(terms), 2)]
        return terms[0]

    nears = half_x - 1
    for k in range(1, half_x):
        device = near(k)
        exchange(0, part.at[lax.rem(device[0], half_x)], row_buf.at[place], device)
    row_buf[place] = part[place]
    negative_grads()
    update(dst_tab, dst_state, dst_acc_out, dest_terms(pack_run, 4))

    all_of(red_recv, 0, row_buf, nears)
    col_buf[mine] = added(row_buf)
    for offset in offsets:
        exchange(1, col_buf.at[mine], col_buf.at[mine], far(offset))

    for c in range(CHUNKS):
        home_copy(c).wait()
    update(src_tab, src_state, src_acc_out, [(pack_own[4 + SRC : 5 + SRC, :], lambda: home_grads[...])])

    all_of(red_recv, 1, col_buf, len(offsets))
    all_buf[place] = added(col_buf)
    for k in range(1, half_x):
        exchange(2, all_buf.at[place], all_buf.at[place], near(k))
    all_of(red_send, 0, row_buf, nears)
    all_of(red_send, 1, col_buf, len(offsets))
    all_of(red_recv, 2, all_buf, nears)
    all_of(red_send, 2, all_buf, nears)
    for i in range(half_x):
        rel_total[i * each : (i + 1) * each, :] = all_buf[i]
    grad = rel_total[...]
    corner = lax.broadcasted_iota(i32, (rels, rels), 0) == lax.broadcasted_iota(i32, (rels, rels), 1)
    state = jnp.sum(jnp.where(corner, rel_acc[...], 0.0), axis=1, keepdims=True)
    state = state + jnp.sum(grad * grad, axis=1, keepdims=True) * (1.0 / width)
    rel_out[...] = relations[...] - relation_rate * grad * lax.rsqrt(state)


def store(*refs):
    count = len(refs) // 2
    sems = refs[-1]
    copies = [pltpu.make_async_copy(refs[i], refs[count + i], sems.at[i]) for i in range(count)]
    for copy in copies:
        copy.start()
    for copy in copies:
        copy.wait()


def solution(mesh):
    nx, ny = mesh.shape["gx"], mesh.shape["gy"]

    def local(src_table, src_acc, dst_table, dst_acc, relations, rel_acc, edge_src, edge_dst, edge_rel, negatives, counts):
        rows, width = src_table.shape
        edges = edge_src.shape[-1]
        negs = negatives.shape[-1]
        rels = relations.shape[0]
        lines = rows // LANES
        vmem = pl.BlockSpec(memory_space=pltpu.VMEM)
        hbm = pl.BlockSpec(memory_space=pltpu.HBM)
        table = jax.ShapeDtypeStruct((rows, width), bf16)
        state = jax.ShapeDtypeStruct((lines, LANES), f32)
        outs = (table, state, table, state, jax.ShapeDtypeStruct((rels, width), f32))
        dma = pltpu.SemaphoreType.DMA
        half, far, each = nx // 2, 2 * ny, rels // (nx // 2)
        inner = pl.pallas_call(
            functools.partial(kernel, (nx, ny)),
            out_shape=outs,
            in_specs=[hbm] * 11,
            out_specs=(vmem,) * 5,
            scratch_shapes=[
                pltpu.VMEM((lines, LANES), f32),
                pltpu.VMEM((lines, LANES), f32),
                pltpu.VMEM((rels, width), f32),
                pltpu.VMEM((1, rels), f32),
                pltpu.VMEM((2, edges), i32),
                pltpu.VMEM((2, edges), i32),
                pltpu.VMEM((2, edges), i32),
                pltpu.VMEM((2, 1, negs), i32),
                pltpu.VMEM((1, 2), i32),
                pltpu.VMEM((lines, LANES), f32),
                pltpu.VMEM((lines, LANES), f32),
                pltpu.VMEM((8, edges), i32),
                pltpu.VMEM((8, edges), i32),
                pltpu.VMEM((8, edges), i32),
                pltpu.VMEM((edges, 8), i32),
                pltpu.VMEM((LANES, width), bf16),
                pltpu.VMEM((LANES, LANES), bf16),
                pltpu.VMEM((edges, width), bf16),
                pltpu.VMEM((edges + negs, width), bf16),
                pltpu.VMEM((edges, width), bf16),
                pltpu.VMEM((edges + negs, width), bf16),
                pltpu.VMEM((edges, width), bf16),
                pltpu.VMEM((edges, negs), bf16),
                pltpu.VMEM((edges, 2 * width), bf16),
                pltpu.VMEM((edges, width), bf16),
                pltpu.VMEM((edges, width), bf16),
                pltpu.VMEM((edges, width), bf16),
                pltpu.VMEM((edges, width), bf16),
                pltpu.VMEM((rels, width), f32),
                pltpu.VMEM((half, each, width), f32),
                pltpu.VMEM((half, each, width), f32),
                pltpu.VMEM((far, each, width), f32),
                pltpu.VMEM((half, each, width), f32),
                pltpu.VMEM((rels, width), f32),
                dma((11,)),
                pltpu.SemaphoreType.REGULAR((7,)),
                dma((2,)),
                dma((2,)),
                dma((CHUNKS,)),
                dma((CHUNKS,)),
                dma((CHUNKS,)),
                dma((CHUNKS,)),
                dma((3,)),
                dma((3,)),
            ],
            compiler_params=pltpu.CompilerParams(collective_id=0, has_side_effects=True, vmem_limit_bytes=40 << 20),
        )(
            *(
                pltpu.with_memory_space_constraint(value, pltpu.HBM)
                for value in (
                    src_table,
                    src_acc.reshape(lines, LANES),
                    dst_table,
                    dst_acc.reshape(lines, LANES),
                    relations,
                    rel_acc.reshape(1, rels),
                    edge_src.reshape(2, edges),
                    edge_dst.reshape(2, edges),
                    edge_rel.reshape(2, edges),
                    negatives.reshape(2, 1, negs),
                    counts.reshape(1, 2),
                )
            )
        )
        out = pl.pallas_call(
            store,
            out_shape=outs,
            in_specs=[vmem] * 5,
            out_specs=(hbm,) * 5,
            scratch_shapes=[dma((5,))],
            compiler_params=pltpu.CompilerParams(vmem_limit_bytes=1 << 20),
        )(*inner)
        return (out[0], out[1].reshape(rows), out[2], out[3].reshape(rows), out[4])

    both = ("gx", "gy")
    listed = P("gx", "gy", None, None)
    return jax.shard_map(
        local,
        mesh=mesh,
        in_specs=(
            P(both, None), P(both), P(both, None), P(both), P(), P(),
            listed, listed, listed, P("gx", "gy", None, None, None), P("gx", "gy", None),
        ),
        out_specs=(P(both, None), P(both), P(both, None), P(both), P()),
        check_vma=False,
    )
```
